32 devices in a mesh: band: 16 (over z, y, core), spin: 2 (over x).
Axes of the slice: x: 2, y: 2, z: 4, core: 2. Of those that a mesh axis runs over, the one named last changes fastest.
Arguments:
- coefficients: bfloat16 [2, 2, 32, 524288], P('spin', None, 'band'), may hold values from -1 to 1
- occupation: int32 [2, 32], P('spin', 'band'), may hold values from 0 to 1000
- miller: int32 [3, 524288], P(None, ('band', 'spin')), may hold values from -8 to 8
- density: float32 [2, 256, 128, 128], P('spin', 'band'), may hold values from 0.25 to 2
- local_factor: float32 [2, 256, 128, 128], P(None, None, 'band'), may hold values from -1.2 to 1.2
Outputs:
- stress: float32 [6], replicated
- kinetic_density: float32 [524288], P(('band', 'spin'))
- gradient_square: float32 [2, 256, 128, 128], P('spin', 'band')
The draws below stay inside these ranges and needn't reach their ends.
All inputs are finite; a program needn't handle non-finite values.
Results may differ from the reference program's by a relative error of at most 0.0003.
Values sent between devices are 32-bit elements; how exact they have to be, the bound alone decides.
No kernel may reach another device: no remote copies, remote signals or barrier semaphores. Data moves between devices by JAX's collectives and lax.ppermute only.
A program may use at most 64 MiB of HBM per device.

```python
import math
import jax
import jax.numpy as jnp
from jax import lax

NPW = 524288
NX = 128
NY = 128
NZ = 256
BANDS = 32
SPINS = 2


def place_ends(result, stream_key, smallest, high):
    longest = result.shape.index(max(result.shape))
    spots = []
    for shift in (0, 1):
        where = [jax.random.randint(jax.random.fold_in(stream_key, axis), (), 0, length) for axis, length in enumerate(result.shape)]
        where[longest] = (where[longest] + shift) % result.shape[longest]
        spots.append(tuple(where))
    return result.at[spots[0]].set(smallest).at[spots[1]].set(high)


def with_spikes(values, rng, source, target, parts, factor):
    def block_of(dim):
        return (jnp.arange(values.shape[dim]) // (values.shape[dim] // parts)).reshape((-1,) + (1,) * (values.ndim - 1 - dim))

    one_side = jax.random.permutation(rng, parts)[block_of(target)]
    other_side = (block_of(target) + parts // 2) % parts
    return jnp.where((block_of(source) == one_side) | (block_of(source) == other_side), factor * values, values)


def steps_of(rng, dims, split, low, largest):
    def one(axis_at, blocks):
        draws = jax.random.uniform(jax.random.fold_in(jax.random.fold_in(rng, 6), axis_at), (blocks,), jnp.float32, low / len(split), largest / len(split))
        return jnp.repeat(jnp.exp(draws), dims[axis_at] // blocks).reshape((-1,) + (1,) * (len(dims) - axis_at - 1))

    level = one(*split[0])
    for cut in split[1:]:
        level = level * one(*cut)
    return level


def bell_draw(rng, dims, deviation, reach, split=(), kind=jnp.bfloat16):
    loudness = steps_of(rng, dims, split, -0.22, 0.18) if split else 1.0
    values = jax.random.normal(rng, dims, jnp.float32) * deviation * loudness
    return jnp.minimum(jnp.maximum(values, -reach), reach).astype(kind)


def heavy_noise(key, shape, width, limit, split, heavy, held_as=jnp.bfloat16):
    entries = width * jax.random.normal(key, shape, jnp.float32)
    if split:
        entries = entries * steps_of(key, shape, split, -0.22, 0.18)
    return jnp.clip(with_spikes(entries, jax.random.fold_in(key, 3), *heavy), -limit, limit).astype(held_as)


def setup_inputs(seed: int = 0) -> dict:
    keys = jax.random.split(jax.random.key(seed), 6)
    coefficients = heavy_noise(keys[0], (SPINS, 2, BANDS, NPW), (2 * BANDS) ** -0.5, 1.0, ((0, 2), (2, 16)), (2, 3, 16, 2.0))
    occupation = place_ends(jax.random.randint(keys[1], (SPINS, BANDS), 0, 1001), jax.random.fold_in(keys[1], 1), 0, 1000).astype(jnp.int32)
    miller = place_ends(jax.random.randint(keys[2], (3, NPW), -8, 9), jax.random.fold_in(keys[2], 1), -8, 8).astype(jnp.int32)
    density = jnp.clip(0.25 + 1.75 * jax.random.uniform(keys[3], (SPINS, NZ, NX, NY), jnp.float32) ** steps_of(keys[3], (SPINS, NZ, NX, NY), ((0, 2), (1, 16)), -0.2, 0.2), 0.25, 2.0)
    local_factor = bell_draw(keys[4], (2, NZ, NX, NY), 0.2, 1.2, ((2, 16),), jnp.float32)
    return {"coefficients": coefficients, "occupation": occupation, "miller": miller, "density": density, "local_factor": local_factor}


occupation_unit = 1000.0
kpoint = (0.25, 0.125, 0.375)
spacing = 0.25


def derivative_table(length):
    row_index = jnp.arange(length, dtype=jnp.int32)[:, None]
    col_index = jnp.arange(length, dtype=jnp.int32)[None, :]
    wrapped = jnp.mod(row_index - col_index, length)
    angles = (jnp.pi / length) * wrapped.astype(jnp.float32)
    on_diagonal = wrapped == 0
    sines = jnp.where(on_diagonal, 1.0, jnp.sin(angles))
    parity = 1.0 - 2.0 * jnp.mod(wrapped, 2).astype(jnp.float32)
    return jnp.where(on_diagonal, 0.0, 0.5 * parity * jnp.cos(angles) / sines).astype(jnp.float32)


def frequencies(length):
    positions = jnp.arange(length, dtype=jnp.int32)
    signed = jnp.where(positions >= length // 2, positions - length, positions)
    return (2.0 * jnp.pi / length) * signed.astype(jnp.float32)


def six_sums(weighting, first_axis, second_axis, third_axis):
    return jnp.stack([
        jnp.sum(weighting * first_axis * first_axis),
        jnp.sum(weighting * second_axis * second_axis),
        jnp.sum(weighting * third_axis * third_axis),
        jnp.sum(weighting * second_axis * third_axis),
        jnp.sum(weighting * first_axis * third_axis),
        jnp.sum(weighting * first_axis * second_axis)])


def reference(coefficients, occupation, miller, density, local_factor):
    highest = lax.Precision.HIGHEST
    weights = occupation.astype(jnp.float32) / occupation_unit
    band_block = math.gcd(BANDS, 32)

    def accumulate(counter, running):
        first_row = (jnp.asarray(counter).astype(jnp.int32) * band_block).astype(jnp.int32)
        piece = lax.dynamic_slice_in_dim(coefficients, first_row, band_block, 2).astype(jnp.float32)
        squares = piece[:, 0] * piece[:, 0] + piece[:, 1] * piece[:, 1]
        weight_piece = lax.dynamic_slice_in_dim(weights, first_row, band_block, 1)
        return running + jnp.einsum('sb,sbg->g', weight_piece, squares, precision=highest)

    kinetic_weight = lax.fori_loop(0, BANDS // band_block, accumulate, jnp.zeros((NPW,), jnp.float32))
    kvec = jnp.array(kpoint, jnp.float32)
    gvec = spacing * (miller.astype(jnp.float32) + kvec[:, None])
    kinetic_density = 0.5 * (gvec[0] ** 2 + gvec[1] ** 2 + gvec[2] ** 2) * kinetic_weight
    kinetic_stress = -six_sums(kinetic_weight, gvec[0], gvec[1], gvec[2]) / NPW

    deriv_x = derivative_table(NX)
    deriv_y = derivative_table(NY)
    deriv_z = derivative_table(NZ)
    grad_x = jnp.einsum('ik,szky->sziy', deriv_x, density, precision=highest)
    grad_y = jnp.einsum('ik,szxk->szxi', deriv_y, density, precision=highest)
    grad_z = jnp.einsum('ik,skxy->sixy', deriv_z, density, precision=highest)
    gradient_square = grad_x * grad_x + grad_y * grad_y + grad_z * grad_z
    kernel = density ** (-1.0 / 3.0) / (1.0 + gradient_square / (4.0 * density * density + 1.0))
    cell_count = NZ * NX * NY
    xc_stress = -six_sums(kernel, grad_x, grad_y, grad_z) / cell_count

    total_density = jnp.sum(density, axis=0)
    spectrum = jnp.fft.fftn(total_density) / cell_count
    real_part = jnp.real(spectrum)
    imag_part = jnp.imag(spectrum)
    freq_z = frequencies(NZ)[:, None, None]
    freq_x = frequencies(NX)[None, :, None]
    freq_y = frequencies(NY)[None, None, :]
    length_sq = freq_x * freq_x + freq_y * freq_y + freq_z * freq_z
    positive = length_sq > 0
    inverse = jnp.where(positive, 1.0 / jnp.where(positive, length_sq, 1.0), 0.0)
    hartree_weight = 4.0 * jnp.pi * (real_part * real_part + imag_part * imag_part) * inverse
    diagonal = jnp.array([1.0, 1.0, 1.0, 0.0, 0.0, 0.0], jnp.float32)
    hartree_stress = 2.0 * six_sums(hartree_weight * inverse, freq_x, freq_y, freq_z) - diagonal * jnp.sum(hartree_weight)
    local_weight = 2.0 * (real_part * local_factor[0] + imag_part * local_factor[1])
    local_stress = six_sums(local_weight, freq_x, freq_y, freq_z)
    stress = kinetic_stress + hartree_stress + local_stress + xc_stress
    return stress, kinetic_density, gradient_square
```

```python
import numpy as np
import jax
import jax.numpy as jnp
from jax import lax
from jax.sharding import PartitionSpec as P

occupation_unit = 1000.0
kpoint = (0.25, 0.125, 0.375)
spacing = 0.25
HIGH = lax.Precision.HIGH


def derivative_table(length):
    wrapped = np.mod(np.arange(length)[:, None] - np.arange(length)[None, :], length)
    angles = np.pi / length * wrapped
    sines = np.where(wrapped == 0, 1.0, np.sin(angles))
    parity = 1.0 - 2.0 * (wrapped % 2)
    return np.where(wrapped == 0, 0.0, 0.5 * parity * np.cos(angles) / sines).astype(np.float32)


def fourier_tables(length):
    phases = np.mod(np.arange(length)[:, None] * np.arange(length)[None, :], length) * (2.0 * np.pi / length)
    return np.cos(phases), np.sin(phases)


def frequencies(length):
    positions = np.arange(length)
    signed = np.where(positions >= length // 2, positions - length, positions)
    return (2.0 * np.pi / length * signed).astype(np.float32)


def halves(values, axis, mine):
    return (
        lax.dynamic_index_in_dim(values, mine, axis, keepdims=False),
        lax.dynamic_index_in_dim(values, 1 - mine, axis, keepdims=False),
    )


def pair_up(size, bit):
    return [(i, i ^ bit) for i in range(size)]


def scatter_sum(values, band_devices, band, spin):
    tail = values.shape[2:]
    spins = values.shape[1]
    bit = 1
    left = band_devices
    done_spin = False
    rest = values.reshape((left, spins) + tail)
    while left > 1:
        mine = (band // bit) % 2
        rest = rest.reshape((left // 2, 2) + rest.shape[1:])
        keep, give = halves(rest, 1, mine)
        rest = keep + lax.ppermute(give, "band", pair_up(band_devices, bit))
        left //= 2
        bit *= 2
        if not done_spin:
            keep, give = halves(rest, 1, spin)
            rest = keep + lax.ppermute(give, "spin", pair_up(spins, 1))
            done_spin = True
    return rest.reshape(tail)


def shards(coefficients, occupation, miller, density, local_factor):
    band_devices = lax.axis_size("band")
    spins = lax.axis_size("spin")
    band = lax.axis_index("band")
    spin = lax.axis_index("spin")
    planes, nx, ny = density.shape[1:]
    nz = planes * band_devices
    rows = nx // band_devices
    cell_count = nz * nx * ny
    waves = coefficients.shape[3]
    dens = density[0]

    dens_send = dens.reshape(planes, band_devices, rows, ny).transpose(1, 0, 2, 3)
    dens_col = lax.all_to_all(dens_send, "band", 0, 0, tiled=True).reshape(nz, rows * ny)

    share = planes // spins
    keep, give = halves(dens.reshape(spins, share, nx, ny), 0, spin)
    total = keep + lax.ppermute(give, "spin", pair_up(spins, 1))

    weights = occupation[0].astype(jnp.float32) / occupation_unit
    piece = coefficients[0].astype(jnp.float32)
    partial = jnp.sum((piece[0] * piece[0] + piece[1] * piece[1]) * weights[:, None], axis=0)
    chunk = waves // (band_devices * spins)
    kinetic_weight = scatter_sum(
        partial.reshape(band_devices, spins, chunk // 128, 128), band_devices, band, spin
    )

    cos_x, sin_x = fourier_tables(nx)
    cos_y, sin_y = fourier_tables(ny)
    cos_z, sin_z = fourier_tables(nz)
    part = ny // spins
    table_y = np.stack(
        [
            np.stack(
                [
                    np.concatenate([cos_y[:, p : p + part], -sin_y[:, p : p + part]], 1),
                    np.concatenate([-sin_y[:, p : p + part], -cos_y[:, p : p + part]], 1),
                ]
            )
            for p in range(0, ny, part)
        ]
    ).astype(np.float32)
    along = jnp.einsum("zxj,pcjm->pczxm", total, table_y, precision=HIGH)
    table_x = np.stack([cos_x, sin_x]).reshape(2, band_devices, rows, nx).astype(np.float32)
    plane = jnp.einsum("cbrj,pczjm->bpzrm", table_x, along, precision=HIGH)
    lanes = plane.shape[-1]
    plane = plane.reshape(band_devices * spins, share, rows, lanes)
    column = lax.all_to_all(plane, ("band", "spin"), 0, 0, tiled=True).reshape(nz, rows * lanes)

    gradz_col = jnp.dot(derivative_table(nz), dens_col, precision=HIGH)
    gradz_back = lax.all_to_all(gradz_col.reshape(band_devices, planes, rows, ny), "band", 0, 0, tiled=True)
    grad_z = gradz_back.transpose(1, 0, 2, 3).reshape(planes, nx, ny)

    first = (jnp.dot((cos_z / cell_count).astype(np.float32), column, precision=HIGH)).reshape(nz, rows, lanes)
    second = (jnp.dot((sin_z / cell_count).astype(np.float32), column, precision=HIGH)).reshape(nz, rows, lanes)
    spectrum = first + jnp.concatenate([second[..., part:], -second[..., :part]], axis=-1)
    factor = lax.dynamic_slice_in_dim(local_factor, spin * part, part, 3)
    factor = jnp.concatenate([factor[0], factor[1]], axis=-1)
    freq_z = jnp.asarray(frequencies(nz))[:, None, None]
    freq_x = lax.dynamic_slice_in_dim(jnp.asarray(frequencies(nx)), band * rows, rows, 0)[:, None]
    freq_y = lax.dynamic_slice_in_dim(jnp.asarray(frequencies(ny)), spin * part, part, 0)
    freq_y = jnp.concatenate([freq_y, freq_y])[None, :]
    length_sq = freq_x * freq_x + freq_y * freq_y + freq_z * freq_z
    positive = length_sq > 0
    inverse = jnp.where(positive, 1.0 / jnp.where(positive, length_sq, 1.0), 0.0)
    hartree = (4.0 * np.pi) * spectrum * spectrum * inverse
    both = 2.0 * (hartree * inverse + spectrum * factor)
    trace = jnp.sum(hartree, axis=0)
    sum_0 = jnp.sum(both, axis=0)
    sum_1 = jnp.sum(both * freq_z, axis=0)
    sum_2 = jnp.sum(both * (freq_z * freq_z), axis=0)
    recip = [
        sum_0 * freq_x * freq_x - trace,
        sum_0 * freq_y * freq_y - trace,
        sum_2 - trace,
        sum_1 * freq_y,
        sum_1 * freq_x,
        sum_0 * freq_x * freq_y,
    ]
    recip = [jnp.sum(r, axis=0) for r in recip]

    deriv_x = derivative_table(nx)
    deriv_y = derivative_table(ny)
    grad_x = jnp.einsum("ik,zky->ziy", deriv_x, dens, precision=HIGH)
    grad_y = jnp.einsum("zxk,ik->zxi", dens, deriv_y, precision=HIGH)
    square = grad_x * grad_x + grad_y * grad_y + grad_z * grad_z
    kernel = dens ** (-1.0 / 3.0) / (1.0 + square / (4.0 * dens * dens + 1.0)) * (-1.0 / cell_count)

    def six(weighting, a, b, c, axes):
        wa, wb = weighting * a, weighting * b
        return [
            jnp.sum(v, axis=axes)
            for v in (wa * a, wb * b, weighting * c * c, wb * c, wa * c, wa * b)
        ]

    xc = six(kernel, grad_x, grad_y, grad_z, (0, 1))

    kvec = jnp.array(kpoint, jnp.float32)
    gvec = spacing * (miller.reshape(3, chunk // 128, 128).astype(jnp.float32) + kvec[:, None, None])
    kinetic_density = 0.5 * (gvec[0] ** 2 + gvec[1] ** 2 + gvec[2] ** 2) * kinetic_weight
    kinetic = six(kinetic_weight * (-1.0 / waves), gvec[0], gvec[1], gvec[2], 0)

    lanewise = jnp.stack([r + x + k for r, x, k in zip(recip, xc, kinetic)])
    stress = jnp.sum(lax.psum(lanewise, ("band", "spin")), axis=1)
    return stress, kinetic_density.reshape(chunk), square[None]


def solution(mesh):
    return jax.shard_map(
        shards,
        mesh=mesh,
        in_specs=(
            P("spin", None, "band", None),
            P("spin", "band"),
            P(None, ("band", "spin")),
            P("spin", "band", None, None),
            P(None, None, "band", None),
        ),
        out_specs=(P(), P(("band", "spin")), P("spin", "band", None, None)),
        check_vma=False,
    )
```

```python
import numpy as np
import jax
import jax.numpy as jnp
from jax import lax
from jax.experimental import pallas as pl
from jax.experimental.pallas import tpu as pltpu
from jax.sharding import PartitionSpec as P

occupation_unit = 1000.0
kpoint = (0.25, 0.125, 0.375)
spacing = 0.25
HIGH = lax.Precision.HIGH


def derivative_table(length):
    wrapped = np.mod(np.arange(length)[:, None] - np.arange(length)[None, :], length)
    angles = np.pi / length * wrapped
    sines = np.where(wrapped == 0, 1.0, np.sin(angles))
    parity = 1.0 - 2.0 * (wrapped % 2)
    return np.where(wrapped == 0, 0.0, 0.5 * parity * np.cos(angles) / sines).astype(np.float32)


def fourier_tables(length):
    phases = np.mod(np.arange(length)[:, None] * np.arange(length)[None, :], length) * (2.0 * np.pi / length)
    return np.cos(phases), np.sin(phases)


def frequencies(length):
    positions = np.arange(length)
    signed = np.where(positions >= length // 2, positions - length, positions)
    return (2.0 * np.pi / length * signed).astype(np.float32)


def halves(values, axis, mine):
    return (
        lax.dynamic_index_in_dim(values, mine, axis, keepdims=False),
        lax.dynamic_index_in_dim(values, 1 - mine, axis, keepdims=False),
    )


def pair_up(size, bit):
    return [(i, i ^ bit) for i in range(size)]


def scatter_sum(values, band_devices, band, spin):
    tail = values.shape[2:]
    spins = values.shape[1]
    bit = 1
    left = band_devices
    done_spin = False
    rest = values.reshape((left, spins) + tail)
    while left > 1:
        mine = (band // bit) % 2
        rest = rest.reshape((left // 2, 2) + rest.shape[1:])
        keep, give = halves(rest, 1, mine)
        rest = keep + lax.ppermute(give, "band", pair_up(band_devices, bit))
        left //= 2
        bit *= 2
        if not done_spin:
            keep, give = halves(rest, 1, spin)
            rest = keep + lax.ppermute(give, "spin", pair_up(spins, 1))
            done_spin = True
    return rest.reshape(tail)


def weigh(weight_ref, coef_ref, out_ref):
    rows = out_ref.shape[0]
    total = jnp.zeros((rows, 128), jnp.float32)
    for n in range(coef_ref.shape[2]):
        real = coef_ref[0, 0, n].astype(jnp.float32).reshape(rows, 128)
        imag = coef_ref[0, 1, n].astype(jnp.float32).reshape(rows, 128)
        total = total + (real * real + imag * imag) * weight_ref[0, n]
    out_ref[...] = total


def occupied_weight(weights, coefficients):
    waves = coefficients.shape[3]
    bands = coefficients.shape[2]
    block = min(waves, 65536 // bands)
    return pl.pallas_call(
        weigh,
        grid=(waves // block,),
        in_specs=[
            pl.BlockSpec(memory_space=pltpu.SMEM),
            pl.BlockSpec((1, 2, bands, block), lambda i: (0, 0, 0, i)),
        ],
        out_specs=pl.BlockSpec((block // 128, 128), lambda i: (i, 0)),
        out_shape=jax.ShapeDtypeStruct((waves // 128, 128), jnp.float32),
        cost_estimate=pl.CostEstimate(
            flops=2000 * waves, bytes_accessed=coefficients.size * 2 + 4 * waves, transcendentals=0
        ),
    )(weights, coefficients)


def shards(coefficients, occupation, miller, density, local_factor):
    band_devices = lax.axis_size("band")
    spins = lax.axis_size("spin")
    band = lax.axis_index("band")
    spin = lax.axis_index("spin")
    planes, nx, ny = density.shape[1:]
    nz = planes * band_devices
    rows = nx // band_devices
    cell_count = nz * nx * ny
    waves = coefficients.shape[3]
    dens = density[0]

    dens_send = dens.reshape(planes, band_devices, rows, ny).transpose(1, 0, 2, 3)
    dens_col = lax.all_to_all(dens_send, "band", 0, 0, tiled=True).reshape(nz, rows * ny)

    share = planes // spins
    keep, give = halves(dens.reshape(spins, share, nx, ny), 0, spin)
    total = keep + lax.ppermute(give, "spin", pair_up(spins, 1))

    weights = occupation.astype(jnp.float32) / occupation_unit
    partial = occupied_weight(weights, coefficients)
    chunk = waves // (band_devices * spins)
    kinetic_weight = scatter_sum(
        partial.reshape(band_devices, spins, chunk // 128, 128), band_devices, band, spin
    )

    cos_x, sin_x = fourier_tables(nx)
    cos_y, sin_y = fourier_tables(ny)
    cos_z, sin_z = fourier_tables(nz)
    part = ny // spins
    table_y = np.stack(
        [
            np.stack(
                [
                    np.concatenate([cos_y[:, p : p + part], -sin_y[:, p : p + part]], 1),
                    np.concatenate([-sin_y[:, p : p + part], -cos_y[:, p : p + part]], 1),
                ]
            )
            for p in range(0, ny, part)
        ]
    ).astype(np.float32)
    along = jnp.einsum("zxj,pcjm->pczxm", total, table_y, precision=HIGH)
    table_x = np.stack([cos_x, sin_x]).reshape(2, band_devices, rows, nx).astype(np.float32)
    plane = jnp.einsum("cbrj,pczjm->bpzrm", table_x, along, precision=HIGH)
    lanes = plane.shape[-1]
    plane = plane.reshape(band_devices * spins, share, rows, lanes)
    column = lax.all_to_all(plane, ("band", "spin"), 0, 0, tiled=True).reshape(nz, rows * lanes)

    gradz_col = jnp.dot(derivative_table(nz), dens_col, precision=HIGH)
    gradz_back = lax.all_to_all(gradz_col.reshape(band_devices, planes, rows, ny), "band", 0, 0, tiled=True)
    grad_z = gradz_back.transpose(1, 0, 2, 3).reshape(planes, nx, ny)

    first = (jnp.dot((cos_z / cell_count).astype(np.float32), column, precision=HIGH)).reshape(nz, rows, lanes)
    second = (jnp.dot((sin_z / cell_count).astype(np.float32), column, precision=HIGH)).reshape(nz, rows, lanes)
    spectrum = first + jnp.concatenate([second[..., part:], -second[..., :part]], axis=-1)
    factor = lax.dynamic_slice_in_dim(local_factor, spin * part, part, 3)
    factor = jnp.concatenate([factor[0], factor[1]], axis=-1)
    freq_z = jnp.asarray(frequencies(nz))[:, None, None]
    freq_x = lax.dynamic_slice_in_dim(jnp.asarray(frequencies(nx)), band * rows, rows, 0)[:, None]
    freq_y = lax.dynamic_slice_in_dim(jnp.asarray(frequencies(ny)), spin * part, part, 0)
    freq_y = jnp.concatenate([freq_y, freq_y])[None, :]
    length_sq = freq_x * freq_x + freq_y * freq_y + freq_z * freq_z
    positive = length_sq > 0
    inverse = jnp.where(positive, 1.0 / jnp.where(positive, length_sq, 1.0), 0.0)
    hartree = (4.0 * np.pi) * spectrum * spectrum * inverse
    both = 2.0 * (hartree * inverse + spectrum * factor)
    trace = jnp.sum(hartree, axis=0)
    sum_0 = jnp.sum(both, axis=0)
    sum_1 = jnp.sum(both * freq_z, axis=0)
    sum_2 = jnp.sum(both * (freq_z * freq_z), axis=0)
    recip = [
        sum_0 * freq_x * freq_x - trace,
        sum_0 * freq_y * freq_y - trace,
        sum_2 - trace,
        sum_1 * freq_y,
        sum_1 * freq_x,
        sum_0 * freq_x * freq_y,
    ]
    recip = [jnp.sum(r, axis=0) for r in recip]

    deriv_x = derivative_table(nx)
    deriv_y = derivative_table(ny)
    grad_x = jnp.einsum("ik,zky->ziy", deriv_x, dens, precision=HIGH)
    grad_y = jnp.einsum("zxk,ik->zxi", dens, deriv_y, precision=HIGH)
    grad_x, grad_y = lax.optimization_barrier((grad_x, grad_y))
    square = grad_x * grad_x + grad_y * grad_y + grad_z * grad_z
    kernel = dens ** (-1.0 / 3.0) / (1.0 + square / (4.0 * dens * dens + 1.0)) * (-1.0 / cell_count)

    def six(weighting, a, b, c, axes):
        wa, wb = weighting * a, weighting * b
        return [
            jnp.sum(v, axis=axes)
            for v in (wa * a, wb * b, weighting * c * c, wb * c, wa * c, wa * b)
        ]

    xc = six(kernel, grad_x, grad_y, grad_z, (0, 1))

    kvec = jnp.array(kpoint, jnp.float32)
    gvec = spacing * (miller.reshape(3, chunk // 128, 128).astype(jnp.float32) + kvec[:, None, None])
    kinetic_density = 0.5 * (gvec[0] ** 2 + gvec[1] ** 2 + gvec[2] ** 2) * kinetic_weight
    kinetic = six(kinetic_weight * (-1.0 / waves), gvec[0], gvec[1], gvec[2], 0)

    lanewise = jnp.stack([r + x + k for r, x, k in zip(recip, xc, kinetic)])
    everywhere = jnp.broadcast_to(lanewise, (band_devices * spins,) + lanewise.shape)
    everywhere = lax.all_to_all(everywhere, ("band", "spin"), 0, 0, tiled=True)
    stress = jnp.sum(everywhere, axis=(0, 2))
    return stress, kinetic_density.reshape(chunk), square[None]


def solution(mesh):
    return jax.shard_map(
        shards,
        mesh=mesh,
        in_specs=(
            P("spin", None, "band", None),
            P("spin", "band"),
            P(None, ("band", "spin")),
            P("spin", "band", None, None),
            P(None, None, "band", None),
        ),
        out_specs=(P(), P(("band", "spin")), P("spin", "band", None, None)),
        check_vma=False,
    )
```

```python
import numpy as np
import jax
import jax.numpy as jnp
from jax import lax
from jax.experimental import pallas as pl
from jax.experimental.pallas import tpu as pltpu
from jax.sharding import PartitionSpec as P

occupation_unit = 1000.0
kpoint = (0.25, 0.125, 0.375)
spacing = 0.25
HIGH = lax.Precision.HIGH


def derivative_table(length):
    wrapped = np.mod(np.arange(length)[:, None] - np.arange(length)[None, :], length)
    angles = np.pi / length * wrapped
    sines = np.where(wrapped == 0, 1.0, np.sin(angles))
    parity = 1.0 - 2.0 * (wrapped % 2)
    return np.where(wrapped == 0, 0.0, 0.5 * parity * np.cos(angles) / sines).astype(np.float32)


def fourier_tables(length):
    phases = np.mod(np.arange(length)[:, None] * np.arange(length)[None, :], length) * (2.0 * np.pi / length)
    return np.cos(phases), np.sin(phases)


def frequencies(length):
    positions = np.arange(length)
    signed = np.where(positions >= length // 2, positions - length, positions)
    return (2.0 * np.pi / length * signed).astype(np.float32)


def halves(values, axis, mine):
    return (
        lax.dynamic_index_in_dim(values, mine, axis, keepdims=False),
        lax.dynamic_index_in_dim(values, 1 - mine, axis, keepdims=False),
    )


def pair_up(size, bit):
    return [(i, i ^ bit) for i in range(size)]


def scatter_start(values, band_devices, band, spin):
    spins = values.shape[1]
    tail = values.shape[2:]
    keep, give = halves(values.reshape((band_devices // 2, 2, spins) + tail), 1, band % 2)
    rest = keep + lax.ppermute(give, "band", pair_up(band_devices, 1))
    keep, give = halves(rest, 1, spin)
    rest = keep + lax.ppermute(give, "spin", pair_up(spins, 1))
    return rest


def scatter_step(rest, bit, band_devices, band, after=None):
    left = rest.shape[0]
    keep, give = halves(rest.reshape((left // 2, 2) + rest.shape[1:]), 1, (band // bit) % 2)
    other = lax.ppermute(give, "band", pair_up(band_devices, bit))
    if after is not None:
        other, after = lax.optimization_barrier((other, after))
    return keep + other, after


def weigh(weight_ref, coef_ref, out_ref):
    rows = out_ref.shape[0]
    total = jnp.zeros((rows, 128), jnp.float32)
    for n in range(coef_ref.shape[2]):
        real = coef_ref[0, 0, n].astype(jnp.float32).reshape(rows, 128)
        imag = coef_ref[0, 1, n].astype(jnp.float32).reshape(rows, 128)
        total = total + (real * real + imag * imag) * weight_ref[0, n]
    out_ref[...] = total


def occupied_weight(weights, coefficients):
    waves = coefficients.shape[3]
    bands = coefficients.shape[2]
    block = min(waves, 65536 // bands)
    return pl.pallas_call(
        weigh,
        grid=(waves // block,),
        in_specs=[
            pl.BlockSpec(memory_space=pltpu.SMEM),
            pl.BlockSpec((1, 2, bands, block), lambda i: (0, 0, 0, i)),
        ],
        out_specs=pl.BlockSpec((block // 128, 128), lambda i: (i, 0)),
        out_shape=jax.ShapeDtypeStruct((waves // 128, 128), jnp.float32),
        cost_estimate=pl.CostEstimate(
            flops=2000 * waves, bytes_accessed=coefficients.size * 2 + 4 * waves, transcendentals=0
        ),
    )(weights, coefficients)


def shards(coefficients, occupation, miller, density, local_factor):
    band_devices = lax.axis_size("band")
    spins = lax.axis_size("spin")
    band = lax.axis_index("band")
    spin = lax.axis_index("spin")
    planes, nx, ny = density.shape[1:]
    nz = planes * band_devices
    rows = nx // band_devices
    cell_count = nz * nx * ny
    waves = coefficients.shape[3]
    dens = density[0]

    dens_send = dens.reshape(planes, band_devices, rows, ny).transpose(1, 0, 2, 3)
    dens_col = lax.all_to_all(dens_send, "band", 0, 0, tiled=True).reshape(nz, rows * ny)

    share = planes // spins
    keep, give = halves(dens.reshape(spins, share, nx, ny), 0, spin)
    total = keep + lax.ppermute(give, "spin", pair_up(spins, 1))

    weights = occupation.astype(jnp.float32) / occupation_unit
    partial = occupied_weight(weights, coefficients)
    chunk = waves // (band_devices * spins)
    first_half = scatter_start(partial.reshape(band_devices, spins, chunk // 128, 128), band_devices, band, spin)

    cos_x, sin_x = fourier_tables(nx)
    cos_y, sin_y = fourier_tables(ny)
    cos_z, sin_z = fourier_tables(nz)
    part = ny // spins
    table_y = np.stack(
        [
            np.stack(
                [
                    np.concatenate([cos_y[:, p : p + part], -sin_y[:, p : p + part]], 1),
                    np.concatenate([-sin_y[:, p : p + part], -cos_y[:, p : p + part]], 1),
                ]
            )
            for p in range(0, ny, part)
        ]
    ).astype(np.float32)
    along = jnp.einsum("zxj,pcjm->pczxm", total, table_y, precision=HIGH)
    table_x = np.stack([cos_x, sin_x]).reshape(2, band_devices, rows, nx).astype(np.float32)
    plane = jnp.einsum("cbrj,pczjm->bpzrm", table_x, along, precision=HIGH)
    lanes = plane.shape[-1]
    plane = plane.reshape(band_devices * spins, share, rows, lanes)
    column = lax.all_to_all(plane, ("band", "spin"), 0, 0, tiled=True).reshape(nz, rows * lanes)

    rest, column = scatter_step(first_half, 2, band_devices, band, column)

    gradz_col = jnp.dot(derivative_table(nz), dens_col, precision=HIGH)
    gradz_back = lax.all_to_all(gradz_col.reshape(band_devices, planes, rows, ny), "band", 0, 0, tiled=True)
    grad_z = gradz_back.transpose(1, 0, 2, 3).reshape(planes, nx, ny)

    first = (jnp.dot((cos_z / cell_count).astype(np.float32), column, precision=HIGH)).reshape(nz, rows, lanes)
    second = (jnp.dot((sin_z / cell_count).astype(np.float32), column, precision=HIGH)).reshape(nz, rows, lanes)
    spectrum = first + jnp.concatenate([second[..., part:], -second[..., :part]], axis=-1)
    local_factor, column = lax.optimization_barrier((local_factor, column))
    factor = lax.dynamic_slice_in_dim(local_factor, spin * part, part, 3)
    factor = jnp.concatenate([factor[0], factor[1]], axis=-1)
    freq_z = jnp.asarray(frequencies(nz))[:, None, None]
    freq_x = lax.dynamic_slice_in_dim(jnp.asarray(frequencies(nx)), band * rows, rows, 0)[:, None]
    freq_y = lax.dynamic_slice_in_dim(jnp.asarray(frequencies(ny)), spin * part, part, 0)
    freq_y = jnp.concatenate([freq_y, freq_y])[None, :]
    length_sq = freq_x * freq_x + freq_y * freq_y + freq_z * freq_z
    positive = length_sq > 0
    inverse = jnp.where(positive, 1.0 / jnp.where(positive, length_sq, 1.0), 0.0)
    hartree = (4.0 * np.pi) * spectrum * spectrum * inverse
    both = 2.0 * (hartree * inverse + spectrum * factor)
    trace = jnp.sum(hartree, axis=0)
    sum_0 = jnp.sum(both, axis=0)
    sum_1 = jnp.sum(both * freq_z, axis=0)
    sum_2 = jnp.sum(both * (freq_z * freq_z), axis=0)
    recip = [
        sum_0 * freq_x * freq_x - trace,
        sum_0 * freq_y * freq_y - trace,
        sum_2 - trace,
        sum_1 * freq_y,
        sum_1 * freq_x,
        sum_0 * freq_x * freq_y,
    ]
    recip = [jnp.sum(r, axis=0) for r in recip]

    deriv_x = derivative_table(nx)
    deriv_y = derivative_table(ny)
    grad_x = jnp.einsum("ik,zky->ziy", deriv_x, dens, precision=HIGH)
    grad_y = jnp.einsum("zxk,ik->zxi", dens, deriv_y, precision=HIGH)
    grad_x, grad_y = lax.optimization_barrier((grad_x, grad_y))
    square = grad_x * grad_x + grad_y * grad_y + grad_z * grad_z
    kernel = dens ** (-1.0 / 3.0) / (1.0 + square / (4.0 * dens * dens + 1.0)) * (-1.0 / cell_count)

    def six(weighting, a, b, c, axes):
        wa, wb = weighting * a, weighting * b
        return [
            jnp.sum(v, axis=axes)
            for v in (wa * a, wb * b, weighting * c * c, wb * c, wa * c, wa * b)
        ]

    xc = six(kernel, grad_x, grad_y, grad_z, (0, 1))

    bit = 4
    while bit < band_devices:
        rest, _ = scatter_step(rest, bit, band_devices, band)
        bit *= 2
    kinetic_weight = rest.reshape(chunk // 128, 128)
    kvec = jnp.array(kpoint, jnp.float32)
    gvec = spacing * (miller.reshape(3, chunk // 128, 128).astype(jnp.float32) + kvec[:, None, None])
    kinetic_density = 0.5 * (gvec[0] ** 2 + gvec[1] ** 2 + gvec[2] ** 2) * kinetic_weight
    kinetic = six(kinetic_weight * (-1.0 / waves), gvec[0], gvec[1], gvec[2], 0)

    lanewise = jnp.stack([r + x + k for r, x, k in zip(recip, xc, kinetic)])
    everywhere = jnp.broadcast_to(lanewise, (band_devices * spins,) + lanewise.shape)
    everywhere = lax.all_to_all(everywhere, ("band", "spin"), 0, 0, tiled=True)
    stress = jnp.sum(everywhere, axis=(0, 2))
    return stress, kinetic_density.reshape(chunk), square[None]


def solution(mesh):
    return jax.shard_map(
        shards,
        mesh=mesh,
        in_specs=(
            P("spin", None, "band", None),
            P("spin", "band"),
            P(None, ("band", "spin")),
            P("spin", "band", None, None),
            P(None, None, "band", None),
        ),
        out_specs=(P(), P(("band", "spin")), P("spin", "band", None, None)),
        check_vma=False,
    )
```
